32 devices in a mesh: loc: 32 (over z, y, x, core).
Axes of the slice: x: 2, y: 2, z: 4, core: 2. Of those that a mesh axis runs over, the one named last changes fastest.
Arguments:
- hazard_bins: int32 [256, 8192], P(None, 'loc'), may hold values from 0 to 63
- curve_index: int32 [8192], P('loc'), may hold values from 0 to 255
- damage_table: float32 [256, 64], replicated, may hold values from 0.02 to 0.9
- insured_value: float32 [8192], P('loc'), may hold values from 0.5 to 5
- deductible: float32 [8192], P('loc'), may hold values from 0.05 to 0.5
- loss_limit: float32 [8192], P('loc'), may hold values from 0.5 to 3
- uncertainty: float32 [128, 8192], P(None, 'loc'), may hold values from 0.5 to 2
- year_ids: int32 [256], replicated, may hold values from 0 to 63
Outputs:
- event_loss: float32 [256, 128], P('loc')
- year_loss: float32 [64, 128], replicated
The draws below stay inside these ranges and needn't reach their ends.
All inputs are finite; a program needn't handle non-finite values.
Results may differ from the reference program's by a relative error of at most 0.00005.
Values sent between devices are 32-bit elements; how exact they have to be, the bound alone decides.
A program may use at most 64 MiB of HBM per device.

```python
import math
import jax
import jax.numpy as jnp
from jax import lax

SAMPLES = 128
YEARS = 64
CURVES = 256
BINS = 64
EVENTS = 256
LOCATIONS = 8192


def plant(drawn, key, smallest, high):
    place = [jax.random.randint(jax.random.fold_in(key, axis), (), 0, length) for axis, length in enumerate(drawn.shape)]
    main_axis = drawn.shape.index(max(drawn.shape))
    beside = place[:main_axis] + [(place[main_axis] + 1) % drawn.shape[main_axis]] + place[main_axis + 1:]
    return drawn.at[tuple(place)].set(smallest).at[tuple(beside)].set(high)


def block_scale(rng, shape, shards, low, top_value):
    def one(dim, blocks):
        draws = jax.random.uniform(jax.random.fold_in(jax.random.fold_in(rng, 6), dim), (blocks,), jnp.float32, low / len(shards), top_value / len(shards))
        return jnp.repeat(jnp.exp(draws), shape[dim] // blocks).reshape((-1,) + (1,) * (len(shape) - dim - 1))

    level = one(*shards[0])
    for cut in shards[1:]:
        level = level * one(*cut)
    return level


def setup_inputs(seed: int = 0) -> dict:
    keys = jax.random.split(jax.random.key(seed), 9)
    hazard_bins = plant(jax.random.randint(keys[0], (EVENTS, LOCATIONS), 0, BINS), jax.random.fold_in(keys[0], 1), 0, BINS - 1).astype(jnp.int32)
    curve_index = plant(jax.random.randint(keys[1], (LOCATIONS,), 0, CURVES), jax.random.fold_in(keys[1], 1), 0, CURVES - 1).astype(jnp.int32)
    damage_table = jnp.clip(jax.random.uniform(keys[2], (CURVES, BINS), jnp.float32, 0.02, 0.9), 0.02, 0.9)
    insured_value = jnp.clip(jnp.exp(math.log(5.0) - 2.3025851 * jax.random.uniform(keys[3], (LOCATIONS,), jnp.float32) ** block_scale(keys[3], (LOCATIONS,), ((0, 32),), -0.2, 0.2)), 0.5, 5.0)
    deductible = jnp.clip(jnp.exp(math.log(0.5) - 2.3025851 * jax.random.uniform(keys[4], (LOCATIONS,), jnp.float32) ** block_scale(keys[4], (LOCATIONS,), ((0, 32),), -0.2, 0.2)), 0.05, 0.5)
    loss_limit = jnp.clip(jnp.exp(math.log(3.0) - 1.7917595 * jax.random.uniform(keys[5], (LOCATIONS,), jnp.float32) ** block_scale(keys[5], (LOCATIONS,), ((0, 32),), -0.2, 0.2)), 0.5, 3.0)
    uncertainty = jnp.clip(jnp.exp(math.log(2.0) - 1.3862944 * jax.random.uniform(keys[6], (SAMPLES, LOCATIONS), jnp.float32) ** block_scale(keys[6], (SAMPLES, LOCATIONS), ((1, 32),), -0.2, 0.2)), 0.5, 2.0)
    year_ids = plant(jax.random.randint(keys[7], (EVENTS,), 0, YEARS), jax.random.fold_in(keys[7], 1), 0, YEARS - 1).astype(jnp.int32)
    return dict(hazard_bins=hazard_bins, curve_index=curve_index, damage_table=damage_table, insured_value=insured_value, deductible=deductible, loss_limit=loss_limit, uncertainty=uncertainty, year_ids=year_ids)


def reference(hazard_bins, curve_index, damage_table, insured_value, deductible, loss_limit, uncertainty, year_ids):
    ratios = damage_table[curve_index[None, :], hazard_bins]
    event_total = hazard_bins.shape[0]
    block_rows = math.gcd(event_total, 128)
    grouped = ratios.reshape(event_total // block_rows, block_rows, ratios.shape[1])

    def block_sum(ratio_block):
        damage = jnp.minimum(ratio_block[:, None, :] * uncertainty[None, :, :], 1.0)
        losses = jnp.minimum(jnp.maximum(insured_value * damage - deductible, 0.0), loss_limit)
        return jnp.sum(losses, axis=2)

    summed = lax.map(block_sum, grouped).reshape(event_total, uncertainty.shape[0])
    event_loss = summed * (1.0 / LOCATIONS)
    membership = (year_ids[:, None] == jnp.arange(YEARS, dtype=jnp.int32)[None, :]).astype(jnp.float32)
    year_loss = jnp.dot(membership.T, event_loss, precision=lax.Precision.HIGHEST, preferred_element_type=jnp.float32) * (YEARS / EVENTS)
    return event_loss, year_loss
```

```python
import functools
import math

import jax
import jax.numpy as jnp
from jax import lax
from jax.experimental import pallas as pl
from jax.experimental.pallas import tpu as pltpu
from jax.sharding import PartitionSpec as P

YEARS = 64
BIN_CHUNK = 8
MESH = pl.DeviceIdType.MESH
F32 = jnp.float32
BF16 = jnp.bfloat16
NT = (((1,), (1,)), ((), ()))


def split3(x):
    a = x.astype(BF16)
    rest = x - a.astype(F32)
    b = rest.astype(BF16)
    c = (rest - b.astype(F32)).astype(BF16)
    return a, b, c


def kernel(
    n,
    group,
    h_ref,
    ci_ref,
    tab_ref,
    iv_ref,
    d_ref,
    lim_ref,
    u_ref,
    yid_ref,
    ev_ref,
    yr_ref,
    hb,
    rt,
    v,
    acc,
    out1,
    in1,
    out2,
    in2,
    out3,
    in3,
    send1,
    recv1,
    send2,
    recv2,
    send3,
    recv3,
):
    planes = n // group
    events, width = h_ref.shape
    samples = u_ref.shape[0]
    curves, bins = tab_ref.shape
    own = events // n
    years = yr_ref.shape[0]
    yown = years // group
    me = lax.axis_index("loc")
    q = me // group
    p = me % group

    def in_group(k):
        return q * group + (p + k) % group

    def in_line(k):
        return ((q + k) % planes) * group + p

    barrier = pltpu.get_barrier_semaphore()
    for k in range(1, group):
        pl.semaphore_signal(barrier, inc=1, device_id=(in_group(k),), device_id_type=MESH)
    for k in range(1, planes):
        pl.semaphore_signal(barrier, inc=1, device_id=(in_line(k),), device_id_type=MESH)

    selector = (
        (lax.broadcasted_iota(jnp.int32, (curves, width), 0) == ci_ref[...])
        .astype(F32)
        .astype(BF16)
    )
    parts = jnp.concatenate(split3(tab_ref[...].T), axis=0)
    picked = jnp.dot(parts, selector, preferred_element_type=F32)
    rt[...] = picked[:bins] + picked[bins : 2 * bins] + picked[2 * bins :]
    v[...] = u_ref[...] * iv_ref[...]
    hb[...] = h_ref[...].astype(F32).astype(BF16)
    acc[...] = jnp.zeros_like(acc)
    cap_row = jnp.maximum(jnp.minimum(lim_ref[...], iv_ref[...] - d_ref[...]), 0.0)
    d_row = d_ref[...]

    @pl.loop(0, bins // BIN_CHUNK)
    def _(c):
        base = pl.multiple_of(c * BIN_CHUNK, BIN_CHUNK)
        rows = rt[pl.ds(base, BIN_CHUNK), :]
        shifted = hb[...] - jnp.full((1, width), base.astype(F32), F32).astype(BF16)
        hots, terms = [], []
        for j in range(BIN_CHUNK):
            x = rows[j : j + 1, :] * v[...] - d_row
            x = jnp.minimum(jnp.maximum(x, 0.0), cap_row)
            hi = x.astype(BF16)
            lo = (x - hi.astype(F32)).astype(BF16)
            terms.append(jnp.concatenate([hi, lo], axis=0))
            hots.append(jnp.where(shifted == BF16(j), BF16(1), BF16(0)))
        acc[...] += lax.dot_general(
            jnp.concatenate(hots, axis=1),
            jnp.concatenate(terms, axis=1),
            NT,
            preferred_element_type=F32,
        )

    scale = 1.0 / (width * n)
    sums = (acc[:, :samples] + acc[:, samples:]) * scale
    member = (
        (lax.broadcasted_iota(jnp.int32, (years, events), 0) == yid_ref[...])
        .astype(F32)
        .astype(BF16)
    )
    ysums = jnp.dot(
        member, jnp.concatenate(split3(sums), axis=1), preferred_element_type=F32
    )
    ysums = ysums[:, :samples] + ysums[:, samples : 2 * samples] + ysums[:, 2 * samples :]
    ysums = ysums * (years / events)
    for t in range(planes):
        for g in range(group):
            at = (t * group + g) * own
            out1[g, t * own : (t + 1) * own, :] = sums[at : at + own, :]
    for g in range(group):
        out1[g, planes * own :, :] = ysums[g * yown : (g + 1) * yown, :]

    pl.semaphore_wait(barrier, group - 1 + planes - 1)

    copies = []
    for k in range(1, group):
        copies.append(
            pltpu.make_async_remote_copy(
                src_ref=out1.at[(p + k) % group],
                dst_ref=in1.at[k - 1],
                send_sem=send1.at[k - 1],
                recv_sem=recv1.at[k - 1],
                device_id=(in_group(k),),
                device_id_type=MESH,
            )
        )
        copies[-1].start()
    total = out1[p]
    for k in range(1, group):
        copies[k - 1].wait_recv()
        total = total + in1[k - 1]

    for t in range(planes):
        out2[t, :own, :] = total[t * own : (t + 1) * own, :]
        out2[t, own:, :] = total[planes * own :, :]
    second = []
    for k in range(1, planes):
        second.append(
            pltpu.make_async_remote_copy(
                src_ref=out2.at[(q + k) % planes],
                dst_ref=in2.at[q],
                send_sem=send2.at[k - 1],
                recv_sem=recv2.at[k - 1],
                device_id=(in_line(k),),
                device_id_type=MESH,
            )
        )
        second[-1].start()
    in2[q] = out2[q]
    for copy in second:
        copy.wait_recv()
    done = in2[0]
    for t in range(1, planes):
        done = done + in2[t]
    out3[...] = done[own:, :]
    third = []
    for k in range(1, group):
        third.append(
            pltpu.make_async_remote_copy(
                src_ref=out3,
                dst_ref=in3.at[p],
                send_sem=send3.at[k - 1],
                recv_sem=recv3.at[k - 1],
                device_id=(in_group(k),),
                device_id_type=MESH,
            )
        )
        third[-1].start()
    ev_ref[...] = done[:own, :]
    in3[p] = done[own:, :]
    for copy in third:
        copy.wait_recv()
    for g in range(group):
        yr_ref[g * yown : (g + 1) * yown, :] = in3[g]
    for copy in copies + second + third:
        copy.wait_send()


def shards(n, hazard, curve, table, value, deductible, limit, uncertainty, year_ids):
    events, width = hazard.shape
    samples = uncertainty.shape[0]
    bins = table.shape[1]
    group = math.gcd(n, 8)
    planes = n // group
    own = events // n
    yown = YEARS // group
    row = lambda a: a.reshape(1, a.shape[0])
    dma = pltpu.SemaphoreType.DMA
    return pl.pallas_call(
        functools.partial(kernel, n, group),
        out_shape=(
            jax.ShapeDtypeStruct((own, samples), F32),
            jax.ShapeDtypeStruct((YEARS, samples), F32),
        ),
        in_specs=[pl.BlockSpec(memory_space=pltpu.VMEM)] * 8,
        out_specs=(pl.BlockSpec(memory_space=pltpu.VMEM),) * 2,
        scratch_shapes=[
            pltpu.VMEM((events, width), BF16),
            pltpu.VMEM((bins, width), F32),
            pltpu.VMEM((samples, width), F32),
            pltpu.VMEM((events, 2 * samples), F32),
            pltpu.VMEM((group, planes * own + yown, samples), F32),
            pltpu.VMEM((group - 1, planes * own + yown, samples), F32),
            pltpu.VMEM((planes, own + yown, samples), F32),
            pltpu.VMEM((planes, own + yown, samples), F32),
            pltpu.VMEM((yown, samples), F32),
            pltpu.VMEM((group, yown, samples), F32),
            dma((group - 1,)),
            dma((group - 1,)),
            dma((planes - 1,)),
            dma((planes - 1,)),
            dma((group - 1,)),
            dma((group - 1,)),
        ],
        compiler_params=pltpu.CompilerParams(collective_id=0, has_side_effects=True),
    )(
        hazard,
        row(curve),
        table,
        row(value),
        row(deductible),
        row(limit),
        uncertainty,
        row(year_ids),
    )


def solution(mesh):
    n = mesh.shape["loc"]
    return jax.shard_map(
        functools.partial(shards, n),
        mesh=mesh,
        in_specs=(P(None, "loc"), P("loc"), P(), P("loc"), P("loc"), P("loc"), P(None, "loc"), P()),
        out_specs=(P("loc", None), P()),
        check_vma=False,
    )
```

```python
import functools
import math

import jax
import jax.numpy as jnp
from jax import lax
from jax.experimental import pallas as pl
from jax.experimental.pallas import tpu as pltpu
from jax.sharding import PartitionSpec as P

YEARS = 64
BIN_CHUNK = 8
MESH = pl.DeviceIdType.MESH
F32 = jnp.float32
BF16 = jnp.bfloat16
NT = (((1,), (1,)), ((), ()))


def split3(x):
    a = x.astype(BF16)
    rest = x - a.astype(F32)
    b = rest.astype(BF16)
    c = (rest - b.astype(F32)).astype(BF16)
    return a, b, c


def kernel(
    n,
    group,
    h_ref,
    ci_ref,
    tab_ref,
    iv_ref,
    d_ref,
    lim_ref,
    u_ref,
    yid_ref,
    ev_ref,
    yr_ref,
    hb,
    rt,
    v,
    acc,
    out1,
    in1,
    out2,
    in2,
    out3,
    in3,
    send1,
    recv1,
    send2,
    recv2,
    send3,
    recv3,
):
    planes = n // group
    events, width = h_ref.shape
    samples = u_ref.shape[0]
    bins, curves = tab_ref.shape
    own = events // n
    years = yr_ref.shape[0]
    yown = years // group
    me = lax.axis_index("loc")
    q = me // group
    p = me % group

    def in_group(k):
        return q * group + (p + k) % group

    def in_line(k):
        return ((q + k) % planes) * group + p

    barrier = pltpu.get_barrier_semaphore()
    for k in range(1, group):
        pl.semaphore_signal(barrier, inc=1, device_id=(in_group(k),), device_id_type=MESH)
    for k in range(1, planes):
        pl.semaphore_signal(barrier, inc=1, device_id=(in_line(k),), device_id_type=MESH)

    selector = (
        (lax.broadcasted_iota(jnp.int32, (curves, width), 0) == ci_ref[...])
        .astype(F32)
        .astype(BF16)
    )
    parts = jnp.concatenate(split3(tab_ref[...]), axis=0)
    picked = jnp.dot(parts, selector, preferred_element_type=F32)
    rt[...] = picked[:bins] + picked[bins : 2 * bins] + picked[2 * bins :]
    v[...] = u_ref[...] * iv_ref[...]
    hb[...] = h_ref[...].astype(F32).astype(BF16)
    acc[...] = jnp.zeros_like(acc)
    cap_row = jnp.maximum(jnp.minimum(lim_ref[...], iv_ref[...] - d_ref[...]), 0.0)
    d_row = d_ref[...]

    @pl.loop(0, bins // BIN_CHUNK)
    def _(c):
        base = pl.multiple_of(c * BIN_CHUNK, BIN_CHUNK)
        rows = rt[pl.ds(base, BIN_CHUNK), :]
        shifted = hb[...] - jnp.full((1, width), base.astype(F32), F32).astype(BF16)
        hots, terms = [], []
        for j in range(BIN_CHUNK):
            x = rows[j : j + 1, :] * v[...] - d_row
            x = jnp.minimum(jnp.maximum(x, 0.0), cap_row)
            hi = x.astype(BF16)
            lo = (x - hi.astype(F32)).astype(BF16)
            terms.append(jnp.concatenate([hi, lo], axis=0))
            hots.append(jnp.where(shifted == BF16(j), BF16(1), BF16(0)))
        acc[...] += lax.dot_general(
            jnp.concatenate(hots, axis=1),
            jnp.concatenate(terms, axis=1),
            NT,
            preferred_element_type=F32,
        )

    scale = 1.0 / (width * n)
    sums = (acc[:, :samples] + acc[:, samples:]) * scale
    member = (
        (lax.broadcasted_iota(jnp.int32, (years, events), 0) == yid_ref[...])
        .astype(F32)
        .astype(BF16)
    )
    ysums = jnp.dot(
        member, jnp.concatenate(split3(sums), axis=1), preferred_element_type=F32
    )
    ysums = ysums[:, :samples] + ysums[:, samples : 2 * samples] + ysums[:, 2 * samples :]
    ysums = ysums * (years / events)
    for t in range(planes):
        for g in range(group):
            at = (t * group + g) * own
            out1[g, t * own : (t + 1) * own, :] = sums[at : at + own, :]
    for g in range(group):
        out1[g, planes * own :, :] = ysums[g * yown : (g + 1) * yown, :]

    pl.semaphore_wait(barrier, group - 1 + planes - 1)

    copies = []
    for k in range(1, group):
        copies.append(
            pltpu.make_async_remote_copy(
                src_ref=out1.at[(p + k) % group],
                dst_ref=in1.at[k - 1],
                send_sem=send1.at[k - 1],
                recv_sem=recv1.at[k - 1],
                device_id=(in_group(k),),
                device_id_type=MESH,
            )
        )
        copies[-1].start()
    total = out1[p]
    for k in range(1, group):
        copies[k - 1].wait_recv()
        total = total + in1[k - 1]

    for t in range(planes):
        out2[t, :own, :] = total[t * own : (t + 1) * own, :]
        out2[t, own:, :] = total[planes * own :, :]
    second = []
    for k in range(1, planes):
        second.append(
            pltpu.make_async_remote_copy(
                src_ref=out2.at[(q + k) % planes],
                dst_ref=in2.at[q],
                send_sem=send2.at[k - 1],
                recv_sem=recv2.at[k - 1],
                device_id=(in_line(k),),
                device_id_type=MESH,
            )
        )
        second[-1].start()
    in2[q] = out2[q]
    for copy in second:
        copy.wait_recv()
    done = in2[0]
    for t in range(1, planes):
        done = done + in2[t]
    out3[...] = done[own:, :]
    third = []
    for k in range(1, group):
        third.append(
            pltpu.make_async_remote_copy(
                src_ref=out3,
                dst_ref=in3.at[p],
                send_sem=send3.at[k - 1],
                recv_sem=recv3.at[k - 1],
                device_id=(in_group(k),),
                device_id_type=MESH,
            )
        )
        third[-1].start()
    ev_ref[...] = done[:own, :]
    in3[p] = done[own:, :]
    for copy in third:
        copy.wait_recv()
    for g in range(group):
        yr_ref[g * yown : (g + 1) * yown, :] = in3[g]
    for copy in copies + second + third:
        copy.wait_send()


def shards(n, hazard, curve, table, value, deductible, limit, uncertainty, year_ids):
    events, width = hazard.shape
    samples = uncertainty.shape[0]
    bins = table.shape[1]
    group = math.gcd(n, 8)
    planes = n // group
    own = events // n
    yown = YEARS // group
    row = lambda a: a.reshape(1, a.shape[0])
    dma = pltpu.SemaphoreType.DMA
    return pl.pallas_call(
        functools.partial(kernel, n, group),
        out_shape=(pltpu.VMEM((own, samples), F32), pltpu.VMEM((YEARS, samples), F32)),
        in_specs=[pl.BlockSpec(memory_space=pltpu.VMEM)] * 8,
        out_specs=(pl.BlockSpec(memory_space=pltpu.VMEM),) * 2,
        scratch_shapes=[
            pltpu.VMEM((events, width), BF16),
            pltpu.VMEM((bins, width), F32),
            pltpu.VMEM((samples, width), F32),
            pltpu.VMEM((events, 2 * samples), F32),
            pltpu.VMEM((group, planes * own + yown, samples), F32),
            pltpu.VMEM((group - 1, planes * own + yown, samples), F32),
            pltpu.VMEM((planes, own + yown, samples), F32),
            pltpu.VMEM((planes, own + yown, samples), F32),
            pltpu.VMEM((yown, samples), F32),
            pltpu.VMEM((group, yown, samples), F32),
            dma((group - 1,)),
            dma((group - 1,)),
            dma((planes - 1,)),
            dma((planes - 1,)),
            dma((group - 1,)),
            dma((group - 1,)),
        ],
        compiler_params=pltpu.CompilerParams(collective_id=0, has_side_effects=True),
    )(
        hazard,
        row(curve),
        table.T,
        row(value),
        row(deductible),
        row(limit),
        uncertainty,
        row(year_ids),
    )


def solution(mesh):
    n = mesh.shape["loc"]
    return jax.shard_map(
        functools.partial(shards, n),
        mesh=mesh,
        in_specs=(P(None, "loc"), P("loc"), P(), P("loc"), P("loc"), P("loc"), P(None, "loc"), P()),
        out_specs=(P("loc", None), P()),
        check_vma=False,
    )
```

```python
import functools
import math

import jax
import jax.numpy as jnp
from jax import lax
from jax.experimental import pallas as pl
from jax.experimental.pallas import tpu as pltpu
from jax.sharding import PartitionSpec as P

YEARS = 64
BIN_CHUNK = 8
MESH = pl.DeviceIdType.MESH
F32 = jnp.float32
BF16 = jnp.bfloat16
NT = (((1,), (1,)), ((), ()))


def split3(x):
    a = x.astype(BF16)
    rest = x - a.astype(F32)
    b = rest.astype(BF16)
    c = (rest - b.astype(F32)).astype(BF16)
    return a, b, c


def kernel(
    n,
    group,
    h_ref,
    ci_ref,
    tab_ref,
    iv_ref,
    d_ref,
    lim_ref,
    u_ref,
    yid_ref,
    ev_ref,
    yr_ref,
    hb,
    rt,
    v,
    acc,
    out1,
    in1,
    out2,
    in2,
    out3,
    in3,
    send1,
    recv1,
    send2,
    recv2,
    send3,
    recv3,
):
    planes = n // group
    events, width = h_ref.shape
    samples = u_ref.shape[0]
    bins, curves = tab_ref.shape
    own = events // n
    years = yr_ref.shape[0]
    yown = years // group
    me = lax.axis_index("loc")
    q = me // group
    p = me % group

    def in_group(k):
        return q * group + (p + k) % group

    def in_line(k):
        return ((q + k) % planes) * group + p

    barrier = pltpu.get_barrier_semaphore()
    for k in range(1, group):
        pl.semaphore_signal(barrier, inc=1, device_id=(in_group(k),), device_id_type=MESH)
    for k in range(1, planes):
        pl.semaphore_signal(barrier, inc=1, device_id=(in_line(k),), device_id_type=MESH)

    selector = (
        (lax.broadcasted_iota(jnp.int32, (curves, width), 0) == ci_ref[...])
        .astype(F32)
        .astype(BF16)
    )
    parts = jnp.concatenate(split3(tab_ref[...]), axis=0)
    picked = jnp.dot(parts, selector, preferred_element_type=F32)
    rt[...] = picked[:bins] + picked[bins : 2 * bins] + picked[2 * bins :]
    v[...] = u_ref[...] * iv_ref[...]
    hb[...] = h_ref[...].astype(F32).astype(BF16)
    acc[...] = jnp.zeros_like(acc)
    cap_row = jnp.maximum(jnp.minimum(lim_ref[...], iv_ref[...] - d_ref[...]), 0.0)
    d_row = d_ref[...]

    @pl.loop(0, bins // BIN_CHUNK)
    def _(c):
        base = pl.multiple_of(c * BIN_CHUNK, BIN_CHUNK)
        rows = rt[pl.ds(base, BIN_CHUNK), :]
        shifted = hb[...] - jnp.full((1, width), base.astype(F32), F32).astype(BF16)
        hots, terms = [], []
        for j in range(BIN_CHUNK):
            x = rows[j : j + 1, :] * v[...] - d_row
            x = jnp.minimum(jnp.maximum(x, 0.0), cap_row)
            hi = x.astype(BF16)
            lo = (x - hi.astype(F32)).astype(BF16)
            terms.append(jnp.concatenate([hi, lo], axis=0))
            hots.append(jnp.where(shifted == BF16(j), BF16(1), BF16(0)))
        acc[...] += lax.dot_general(
            jnp.concatenate(hots, axis=1),
            jnp.concatenate(terms, axis=1),
            NT,
            preferred_element_type=F32,
        )

    scale = 1.0 / (width * n)
    sums = (acc[:, :samples] + acc[:, samples:]) * scale
    member = (
        (lax.broadcasted_iota(jnp.int32, (years, events), 0) == yid_ref[...])
        .astype(F32)
        .astype(BF16)
    )
    ysums = jnp.dot(
        member, jnp.concatenate(split3(sums), axis=1), preferred_element_type=F32
    )
    ysums = ysums[:, :samples] + ysums[:, samples : 2 * samples] + ysums[:, 2 * samples :]
    ysums = ysums * (years / events)
    for t in range(planes):
        for g in range(group):
            at = (t * group + g) * own
            out1[g, t * own : (t + 1) * own, :] = sums[at : at + own, :]
    for g in range(group):
        out1[g, planes * own :, :] = ysums[g * yown : (g + 1) * yown, :]

    pl.semaphore_wait(barrier, group - 1 + planes - 1)

    cut = planes * own
    event_rows, year_rows = pl.ds(0, cut), pl.ds(cut, yown)
    event_row, year_row = pl.ds(0, own), pl.ds(own, yown)

    def to_group(rows, first):
        sent = []
        for k in range(1, group):
            sent.append(
                pltpu.make_async_remote_copy(
                    src_ref=out1.at[(p + k) % group, rows],
                    dst_ref=in1.at[k - 1, rows],
                    send_sem=send1.at[first + k - 1],
                    recv_sem=recv1.at[first + k - 1],
                    device_id=(in_group(k),),
                    device_id_type=MESH,
                )
            )
            sent[-1].start()
        return sent

    def to_line(rows, first):
        sent = []
        for k in range(1, planes):
            sent.append(
                pltpu.make_async_remote_copy(
                    src_ref=out2.at[(q + k) % planes, rows],
                    dst_ref=in2.at[q, rows],
                    send_sem=send2.at[first + k - 1],
                    recv_sem=recv2.at[first + k - 1],
                    device_id=(in_line(k),),
                    device_id_type=MESH,
                )
            )
            sent[-1].start()
        return sent

    def group_sum(rows, sent):
        total = out1[p, rows]
        for k in range(1, group):
            sent[k - 1].wait_recv()
            total = total + in1[k - 1, rows]
        return total

    def line_sum(rows, sent):
        in2[q, rows] = out2[q, rows]
        for copy in sent:
            copy.wait_recv()
        total = in2[0, rows]
        for t in range(1, planes):
            total = total + in2[t, rows]
        return total

    years1 = to_group(year_rows, 0)
    events1 = to_group(event_rows, group - 1)
    total = group_sum(year_rows, years1)
    for t in range(planes):
        out2[t, own:, :] = total
    years2 = to_line(year_row, 0)
    total = group_sum(event_rows, events1)
    for t in range(planes):
        out2[t, :own, :] = total[t * own : (t + 1) * own, :]
    events2 = to_line(event_row, planes - 1)
    year_done = line_sum(year_row, years2)
    out3[...] = year_done
    third = []
    for k in range(1, group):
        third.append(
            pltpu.make_async_remote_copy(
                src_ref=out3,
                dst_ref=in3.at[p],
                send_sem=send3.at[k - 1],
                recv_sem=recv3.at[k - 1],
                device_id=(in_group(k),),
                device_id_type=MESH,
            )
        )
        third[-1].start()
    in3[p] = year_done
    ev_ref[...] = line_sum(event_row, events2)
    for copy in third:
        copy.wait_recv()
    for g in range(group):
        yr_ref[g * yown : (g + 1) * yown, :] = in3[g]
    for copy in years1 + events1 + years2 + events2 + third:
        copy.wait_send()


def shards(n, hazard, curve, table, value, deductible, limit, uncertainty, year_ids):
    events, width = hazard.shape
    samples = uncertainty.shape[0]
    bins = table.shape[1]
    group = math.gcd(n, 8)
    planes = n // group
    own = events // n
    yown = YEARS // group
    row = lambda a: a.reshape(1, a.shape[0])
    dma = pltpu.SemaphoreType.DMA
    return pl.pallas_call(
        functools.partial(kernel, n, group),
        out_shape=(pltpu.VMEM((own, samples), F32), pltpu.VMEM((YEARS, samples), F32)),
        in_specs=[pl.BlockSpec(memory_space=pltpu.VMEM)] * 8,
        out_specs=(pl.BlockSpec(memory_space=pltpu.VMEM),) * 2,
        scratch_shapes=[
            pltpu.VMEM((events, width), BF16),
            pltpu.VMEM((bins, width), F32),
            pltpu.VMEM((samples, width), F32),
            pltpu.VMEM((events, 2 * samples), F32),
            pltpu.VMEM((group, planes * own + yown, samples), F32),
            pltpu.VMEM((group - 1, planes * own + yown, samples), F32),
            pltpu.VMEM((planes, own + yown, samples), F32),
            pltpu.VMEM((planes, own + yown, samples), F32),
            pltpu.VMEM((yown, samples), F32),
            pltpu.VMEM((group, yown, samples), F32),
            dma((2 * (group - 1),)),
            dma((2 * (group - 1),)),
            dma((2 * (planes - 1),)),
            dma((2 * (planes - 1),)),
            dma((group - 1,)),
            dma((group - 1,)),
        ],
        compiler_params=pltpu.CompilerParams(collective_id=0, has_side_effects=True),
    )(
        hazard,
        row(curve),
        table.T,
        row(value),
        row(deductible),
        row(limit),
        uncertainty,
        row(year_ids),
    )


def solution(mesh):
    n = mesh.shape["loc"]
    return jax.shard_map(
        functools.partial(shards, n),
        mesh=mesh,
        in_specs=(P(None, "loc"), P("loc"), P(), P("loc"), P("loc"), P("loc"), P(None, "loc"), P()),
        out_specs=(P("loc", None), P()),
        check_vma=False,
    )
```

```python
import functools
import math

import jax
import jax.numpy as jnp
from jax import lax
from jax.experimental import pallas as pl
from jax.experimental.pallas import tpu as pltpu
from jax.sharding import PartitionSpec as P

YEARS = 64
BIN_CHUNK = 8
MESH = pl.DeviceIdType.MESH
F32 = jnp.float32
BF16 = jnp.bfloat16
NT = (((1,), (1,)), ((), ()))


def split3(x):
    a = x.astype(BF16)
    rest = x - a.astype(F32)
    b = rest.astype(BF16)
    c = (rest - b.astype(F32)).astype(BF16)
    return a, b, c


def far_first(count):
    return sorted(range(count), key=lambda k: abs(2 * k + 1 - count))


def kernel(
    n,
    group,
    h_ref,
    ci_ref,
    tab_ref,
    iv_ref,
    d_ref,
    lim_ref,
    u_ref,
    yid_ref,
    ev_ref,
    yr_ref,
    hb,
    rt,
    v,
    acc,
    out1,
    in1,
    out2,
    in2,
    out3,
    in3,
    send1,
    recv1,
    send2,
    recv2,
    send3,
    recv3,
):
    planes = n // group
    events, width = h_ref.shape
    samples = u_ref.shape[0]
    bins, curves = tab_ref.shape
    own = events // n
    years = yr_ref.shape[0]
    yown = years // group
    me = lax.axis_index("loc")
    q = me // group
    p = me % group

    def in_group(k):
        return q * group + (p + k) % group

    def in_line(k):
        return ((q + k) % planes) * group + p

    barrier = pltpu.get_barrier_semaphore()
    for k in range(1, group):
        pl.semaphore_signal(barrier, inc=1, device_id=(in_group(k),), device_id_type=MESH)
    for k in range(1, planes):
        pl.semaphore_signal(barrier, inc=1, device_id=(in_line(k),), device_id_type=MESH)

    selector = (
        (lax.broadcasted_iota(jnp.int32, (curves, width), 0) == ci_ref[...])
        .astype(F32)
        .astype(BF16)
    )
    parts = jnp.concatenate(split3(tab_ref[...]), axis=0)
    picked = jnp.dot(parts, selector, preferred_element_type=F32)
    rt[...] = picked[:bins] + picked[bins : 2 * bins] + picked[2 * bins :]
    v[...] = u_ref[...] * iv_ref[...]
    hb[...] = h_ref[...].astype(F32).astype(BF16)
    acc[...] = jnp.zeros_like(acc)
    cap_row = jnp.maximum(jnp.minimum(lim_ref[...], iv_ref[...] - d_ref[...]), 0.0)
    d_row = d_ref[...]

    @pl.loop(0, bins // BIN_CHUNK)
    def _(c):
        base = pl.multiple_of(c * BIN_CHUNK, BIN_CHUNK)
        rows = rt[pl.ds(base, BIN_CHUNK), :]
        shifted = hb[...] - jnp.full((1, width), base.astype(F32), F32).astype(BF16)
        hots, terms = [], []
        for j in range(BIN_CHUNK):
            x = rows[j : j + 1, :] * v[...] - d_row
            x = jnp.minimum(jnp.maximum(x, 0.0), cap_row)
            hi = x.astype(BF16)
            lo = (x - hi.astype(F32)).astype(BF16)
            terms.append(jnp.concatenate([hi, lo], axis=0))
            hots.append(jnp.where(shifted == BF16(j), BF16(1), BF16(0)))
        acc[...] += lax.dot_general(
            jnp.concatenate(hots, axis=1),
            jnp.concatenate(terms, axis=1),
            NT,
            preferred_element_type=F32,
        )

    scale = 1.0 / (width * n)
    sums = (acc[:, :samples] + acc[:, samples:]) * scale
    member = (
        (lax.broadcasted_iota(jnp.int32, (years, events), 0) == yid_ref[...])
        .astype(F32)
        .astype(BF16)
    )
    ysums = jnp.dot(
        member, jnp.concatenate(split3(sums), axis=1), preferred_element_type=F32
    )
    ysums = ysums[:, :samples] + ysums[:, samples : 2 * samples] + ysums[:, 2 * samples :]
    ysums = ysums * (years / events)
    for t in range(planes):
        for g in range(group):
            at = (t * group + g) * own
            out1[g, t * own : (t + 1) * own, :] = sums[at : at + own, :]
    for g in range(group):
        out1[g, planes * own :, :] = ysums[g * yown : (g + 1) * yown, :]

    pl.semaphore_wait(barrier, group - 1 + planes - 1)

    cut = planes * own
    event_rows, year_rows = pl.ds(0, cut), pl.ds(cut, yown)
    event_row, year_row = pl.ds(0, own), pl.ds(own, yown)

    def to_group(rows, first):
        sent = []
        for k in range(1, group):
            sent.append(
                pltpu.make_async_remote_copy(
                    src_ref=out1.at[(p + k) % group, rows],
                    dst_ref=in1.at[k - 1, rows],
                    send_sem=send1.at[first + k - 1],
                    recv_sem=recv1.at[first + k - 1],
                    device_id=(in_group(k),),
                    device_id_type=MESH,
                )
            )
        for k in far_first(len(sent)):
            sent[k].start()
        return sent

    def to_line(rows, first):
        sent = []
        for k in range(1, planes):
            sent.append(
                pltpu.make_async_remote_copy(
                    src_ref=out2.at[(q + k) % planes, rows],
                    dst_ref=in2.at[q, rows],
                    send_sem=send2.at[first + k - 1],
                    recv_sem=recv2.at[first + k - 1],
                    device_id=(in_line(k),),
                    device_id_type=MESH,
                )
            )
        for k in far_first(len(sent)):
            sent[k].start()
        return sent

    def group_sum(rows, sent):
        total = out1[p, rows]
        for k in range(1, group):
            sent[k - 1].wait_recv()
            total = total + in1[k - 1, rows]
        return total

    def line_sum(rows, sent):
        in2[q, rows] = out2[q, rows]
        for copy in sent:
            copy.wait_recv()
        total = in2[0, rows]
        for t in range(1, planes):
            total = total + in2[t, rows]
        return total

    years1 = to_group(year_rows, 0)
    events1 = to_group(event_rows, group - 1)
    total = group_sum(year_rows, years1)
    for t in range(planes):
        out2[t, own:, :] = total
    years2 = to_line(year_row, 0)
    total = group_sum(event_rows, events1)
    for t in range(planes):
        out2[t, :own, :] = total[t * own : (t + 1) * own, :]
    events2 = to_line(event_row, planes - 1)
    year_done = line_sum(year_row, years2)
    out3[...] = year_done
    third = []
    for k in range(1, group):
        third.append(
            pltpu.make_async_remote_copy(
                src_ref=out3,
                dst_ref=in3.at[p],
                send_sem=send3.at[k - 1],
                recv_sem=recv3.at[k - 1],
                device_id=(in_group(k),),
                device_id_type=MESH,
            )
        )
    for k in far_first(len(third)):
        third[k].start()
    in3[p] = year_done
    ev_ref[...] = line_sum(event_row, events2)
    for copy in third:
        copy.wait_recv()
    for g in range(group):
        yr_ref[g * yown : (g + 1) * yown, :] = in3[g]
    for copy in years1 + events1 + years2 + events2 + third:
        copy.wait_send()


def shards(n, hazard, curve, table, value, deductible, limit, uncertainty, year_ids):
    events, width = hazard.shape
    samples = uncertainty.shape[0]
    bins = table.shape[1]
    group = math.gcd(n, 8)
    planes = n // group
    own = events // n
    yown = YEARS // group
    row = lambda a: a.reshape(1, a.shape[0])
    dma = pltpu.SemaphoreType.DMA
    return pl.pallas_call(
        functools.partial(kernel, n, group),
        out_shape=(pltpu.VMEM((own, samples), F32), pltpu.VMEM((YEARS, samples), F32)),
        in_specs=[pl.BlockSpec(memory_space=pltpu.VMEM)] * 8,
        out_specs=(pl.BlockSpec(memory_space=pltpu.VMEM),) * 2,
        scratch_shapes=[
            pltpu.VMEM((events, width), BF16),
            pltpu.VMEM((bins, width), F32),
            pltpu.VMEM((samples, width), F32),
            pltpu.VMEM((events, 2 * samples), F32),
            pltpu.VMEM((group, planes * own + yown, samples), F32),
            pltpu.VMEM((group - 1, planes * own + yown, samples), F32),
            pltpu.VMEM((planes, own + yown, samples), F32),
            pltpu.VMEM((planes, own + yown, samples), F32),
            pltpu.VMEM((yown, samples), F32),
            pltpu.VMEM((group, yown, samples), F32),
            dma((2 * (group - 1),)),
            dma((2 * (group - 1),)),
            dma((2 * (planes - 1),)),
            dma((2 * (planes - 1),)),
            dma((group - 1,)),
            dma((group - 1,)),
        ],
        compiler_params=pltpu.CompilerParams(collective_id=0, has_side_effects=True),
    )(
        hazard,
        row(curve),
        table.T,
        row(value),
        row(deductible),
        row(limit),
        uncertainty,
        row(year_ids),
    )


def solution(mesh):
    n = mesh.shape["loc"]
    return jax.shard_map(
        functools.partial(shards, n),
        mesh=mesh,
        in_specs=(P(None, "loc"), P("loc"), P(), P("loc"), P("loc"), P("loc"), P(None, "loc"), P()),
        out_specs=(P("loc", None), P()),
        check_vma=False,
    )
```
